32 devices in a mesh: data: 4 (over y, z), ctx: 8 (over x, core).
Axes of the slice: x: 4, y: 2, z: 2, core: 2. Of those that a mesh axis runs over, the one named last changes fastest.
The devices are a block of a 4x4x8 slice.
Arguments:
- queries: bfloat16 [32, 6144, 3, 128], P('data', 'ctx'), parts along dimension 0
- keys_in: bfloat16 [32, 6144, 1, 128], P('data', 'ctx'), parts along dimension 0
- values_in: bfloat16 [32, 6144, 1, 128], P('data', 'ctx'), parts along dimension 0
- grad_out: bfloat16 [32, 6144, 3, 128], P('data', 'ctx'), parts along dimension 0
Outputs:
- output 1: bfloat16 [32, 6144, 3, 128], P('data', 'ctx'), parts along dimension 0
- output 2: bfloat16 [32, 6144, 3, 128], P('data', 'ctx'), parts along dimension 0
- output 3: bfloat16 [32, 6144, 1, 128], P('data', 'ctx'), parts along dimension 0
- output 4: bfloat16 [32, 6144, 1, 128], P('data', 'ctx'), parts along dimension 0
There are 4 independent parts. The reference program is written for one: setup_inputs(seed, part) draws one part's arguments, and reference() takes and returns one part's arrays. A program takes and returns all parts, laid end to end along the dimension named above; each array names one.
All inputs are finite; a program needn't handle non-finite values.
Results may differ from the reference program's by a relative error of at most 0.0171527.
Values are sent between devices in bfloat16 or wider.
A program may use at most 768 MiB of HBM per device.

```python
import jax
import jax.numpy as jnp
from jax import lax

BATCH = 8
TOKENS_DEV = 768
CTX_DEVICES = 8
Q_LOCAL = 3
KV_LOCAL = 1
HEAD_DIM = 128

SEQ_LEN = CTX_DEVICES * TOKENS_DEV
HALF_LEN = TOKENS_DEV // 2
NUM_PIECES = 2 * CTX_DEVICES
GROUP_SIZE = Q_LOCAL // KV_LOCAL
SPREAD = 1.6


def true_positions():
    token_index = jnp.arange(SEQ_LEN, dtype=jnp.int32)
    shard_id = token_index // TOKENS_DEV
    offset = token_index % TOKENS_DEV
    low_pos = shard_id * HALF_LEN + offset
    high_pos = (NUM_PIECES - 1 - shard_id) * HALF_LEN + offset - HALF_LEN
    return jnp.where(offset < HALF_LEN, low_pos, high_pos)


def setup_inputs(seed: int = 0, part: int = 0) -> dict:
    base_key = jax.random.fold_in(jax.random.key(seed), part)
    key_q, key_k, key_v, key_g = jax.random.split(base_key, 4)
    q_shape = (BATCH, SEQ_LEN, Q_LOCAL, HEAD_DIM)
    kv_shape = (BATCH, SEQ_LEN, KV_LOCAL, HEAD_DIM)
    queries = SPREAD * jax.random.normal(key_q, q_shape, jnp.float32)
    keys_in = SPREAD * jax.random.normal(key_k, kv_shape, jnp.float32)
    values_in = jax.random.normal(key_v, kv_shape, jnp.float32)
    grad_out = jax.random.normal(key_g, q_shape, jnp.float32)
    return {"queries": queries.astype(jnp.bfloat16), "keys_in": keys_in.astype(jnp.bfloat16), "values_in": values_in.astype(jnp.bfloat16), "grad_out": grad_out.astype(jnp.bfloat16)}


def reference(queries, keys_in, values_in, grad_out):
    score_scale = HEAD_DIM ** -0.5
    positions = true_positions()
    block_pos = positions.reshape(NUM_PIECES, HALF_LEN)
    keys_wide = keys_in.astype(jnp.float32)
    values_wide = values_in.astype(jnp.float32)

    def to_blocks(tensor):
        return tensor.reshape(BATCH, NUM_PIECES, HALF_LEN, KV_LOCAL, GROUP_SIZE, HEAD_DIM).transpose(1, 0, 2, 3, 4, 5)

    def from_blocks(tensor):
        return tensor.transpose(1, 0, 2, 3, 4, 5).reshape(BATCH, SEQ_LEN, Q_LOCAL, HEAD_DIM)

    def masked_scores(q_blk, pos_blk):
        raw_scores = jnp.einsum("bqhgd,bkhd->bhgqk", q_blk.astype(jnp.float32), keys_wide) * score_scale
        visible = pos_blk[:, None] >= positions[None, :]
        return jnp.where(visible, raw_scores, -jnp.inf)

    def forward_block(blk_args):
        q_blk, pos_blk = blk_args
        masked = masked_scores(q_blk, pos_blk)
        row_max = jnp.max(masked, axis=-1)
        row_sum = jnp.sum(jnp.exp(masked - row_max[..., None]), axis=-1)
        log_sum = row_max + jnp.log(row_sum)
        prob_tile = jnp.exp(masked - log_sum[..., None]).astype(jnp.bfloat16).astype(jnp.float32)
        out_blk = jnp.einsum("bhgqk,bkhd->bqhgd", prob_tile, values_wide)
        return out_blk.astype(jnp.bfloat16), log_sum

    q_blocks = to_blocks(queries)
    g_blocks = to_blocks(grad_out)
    out_blocks, lse_blocks = lax.map(forward_block, (q_blocks, block_pos))
    d_rows = jnp.einsum("nbqhgd,nbqhgd->nbhgq", g_blocks.astype(jnp.float32), out_blocks.astype(jnp.float32))

    def backward_step(loop_carry, blk_args):
        dk_acc, dv_acc = loop_carry
        q_blk, g_blk, lse_blk, drow_blk, pos_blk = blk_args
        q_wide = q_blk.astype(jnp.float32)
        g_wide = g_blk.astype(jnp.float32)
        prob_tile = jnp.exp(masked_scores(q_blk, pos_blk) - lse_blk[..., None])
        prob_low = prob_tile.astype(jnp.bfloat16).astype(jnp.float32)
        dv_acc = dv_acc + jnp.einsum("bhgqk,bqhgd->bkhd", prob_low, g_wide)
        dprob_tile = jnp.einsum("bqhgd,bkhd->bhgqk", g_wide, values_wide)
        dscore_tile = (prob_tile * (dprob_tile - drow_blk[..., None])).astype(jnp.bfloat16).astype(jnp.float32)
        dq_blk = jnp.einsum("bhgqk,bkhd->bqhgd", dscore_tile, keys_wide) * score_scale
        dk_acc = dk_acc + jnp.einsum("bhgqk,bqhgd->bkhd", dscore_tile, q_wide) * score_scale
        return (dk_acc, dv_acc), dq_blk.astype(jnp.bfloat16)

    zeros_kv = jnp.zeros((BATCH, SEQ_LEN, KV_LOCAL, HEAD_DIM), jnp.float32)
    grads_kv, dq_blocks = lax.scan(backward_step, (zeros_kv, zeros_kv), (q_blocks, g_blocks, lse_blocks, d_rows, block_pos))
    return (from_blocks(out_blocks), from_blocks(dq_blocks), grads_kv[0].astype(jnp.bfloat16), grads_kv[1].astype(jnp.bfloat16))
```

```python
import functools
import math

import jax
import jax.numpy as jnp
from jax import lax
from jax.experimental import pallas as pl
from jax.experimental.pallas import tpu as pltpu
from jax.sharding import PartitionSpec as P

f32=jnp.float32; bf16=jnp.bfloat16
NEG=-1e30
R=256
def rowcol(n):
    return lax.broadcasted_iota(jnp.int32,(n,n),0), lax.broadcasted_iota(jnp.int32,(n,n),1)

class Core:
    def __init__(s, seg, nseg, d):
        s.seg=seg; s.ns=nseg; s.d=d; s.nr=seg//R; s.c=(d**-0.5)*math.log2(math.e)
    def at(s, i, r=None):
        if r is None: return pl.ds(pl.multiple_of(i*s.seg, s.seg), s.seg)
        return pl.ds(pl.multiple_of(i*s.seg+r*R, R), R)
    def fa(s, kb, qT, sb, mb, qi, ki, diag, r, c, m):
        cs=slice(r*R,(r+1)*R); rs=slice(c*R,(c+1)*R)
        if diag and c>r: return m
        x=jnp.dot(kb[s.at(ki,c),:], qT[:, s.at(qi,r)], preferred_element_type=f32)
        if diag and c==r:
            ri,ci=rowcol(R)
            x=jnp.where(ri<=ci, x, NEG)
        sb[rs,cs]=x
        x=jnp.max(x,axis=0,keepdims=True)
        m=x if m is None else jnp.maximum(m,x)
        if c==(r if diag else s.nr-1): mb[:,cs]=m
        return m
    def fb(s, vT, sb, mb, acc, ms, ls, sel, ki, diag, r, c, cx):
        cs=slice(r*R,(r+1)*R); rs=slice(c*R,(c+1)*R)
        if diag and c>r: return cx
        if c==0:
            mn=mb[:,cs]*s.c
            if not diag: mn=jnp.maximum(ms[sel,:,cs],mn)
        else: mn,l0,o0=cx
        p=jnp.exp2(sb[rs,cs]*s.c-mn)
        l=jnp.sum(p,axis=0,keepdims=True)
        o=jnp.dot(vT[:,s.at(ki,c)], p.astype(bf16), preferred_element_type=f32)
        if c: l=l0+l; o=o0+o
        if c==(r if diag else s.nr-1):
            if not diag:
                al=jnp.exp2(ms[sel,:,cs]-mn)
                l=l+ls[sel,:,cs]*al
                o=o+acc[sel,:,cs]*al
            ms[sel,:,cs]=mn; ls[sel,:,cs]=l; acc[sel,:,cs]=o
        return mn,l,o
    def ba(s, q, do, kT, vT, lsc, dsc, bufs, qi, sel, ki, diag, r):
        pb,db,tb=bufs
        rs=slice(r*R,(r+1)*R)
        n=(r+1)*R if diag else s.seg
        ks=pl.ds(pl.multiple_of(ki*s.seg,s.seg),n)
        x=jnp.dot(q[s.at(qi,r),:], kT[:,ks], preferred_element_type=f32)
        dp=jnp.dot(do[s.at(qi,r),:], vT[:,ks], preferred_element_type=f32)
        l=jnp.concatenate([lsc[sel,rs,:]]*(n//128),axis=1)
        dd=jnp.concatenate([dsc[sel,rs,:]]*(n//128),axis=1)
        p=jnp.exp2(x*s.c-l)
        if diag:
            ri,ci=rowcol(R)
            t=jnp.where(ri>=ci,p[:,r*R:],0.0)
            p=jnp.concatenate([p[:,:r*R],t],axis=1) if r else t
        ds=(p*(dp-dd)).astype(bf16)
        pb[rs,:n]=p.astype(bf16); db[rs,:n]=ds
        tb[:n,rs]=ds.T
    def bb(s, qT, doT, kT, dqT, dkT, dvT, bufs, qi, sel, ki, diag, r, cx):
        pb,db,tb=bufs
        rs=slice(r*R,(r+1)*R)
        n=(r+1)*R if diag else s.seg
        ks=pl.ds(pl.multiple_of(ki*s.seg,s.seg),n)
        dot=lambda a,b: jnp.dot(a,b,preferred_element_type=f32)
        x=dot(doT[:,s.at(qi,r)], pb[rs,:n])
        y=dot(qT[:,s.at(qi,r)], db[rs,:n])
        z=dot(kT[:,ks], tb[:n,rs])
        cols=slice(r*R,(r+1)*R)
        if diag:
            dqT[sel,:,cols]=z
            dvT[:,ks]+=x; dkT[:,ks]+=y
            return None
        dqT[sel,:,cols]+=z
        x,y=(x,y) if cx is None else (cx[0]+x,cx[1]+y)
        if r==s.nr-1:
            dvT[:,ks]+=x; dkT[:,ks]+=y
        return x,y
    def steps(s, y):
        a=y; b=s.ns-1-y
        out=[(0,a,a,True),(1,b,b,True)]
        for t in range(s.ns-1):
            early = t<y
            out.append((jnp.where(early,0,1), jnp.where(early,a,b), jnp.where(early,t,t-y), False))
        return out
    def forward(s, y, kb, vT, qT, oT, lse, sbs, mbs, acc, ms, ls):
        st=s.steps(y)
        def A(t,r,c,m): sel,qi,ki,dg=st[t]; return s.fa(kb,qT,sbs[t%2],mbs[t%2],qi,ki,dg,r,c,m)
        def B(t,r,c,cx): sel,qi,ki,dg=st[t]; return s.fb(vT,sbs[t%2],mbs[t%2],acc,ms,ls,sel,ki,dg,r,c,cx)
        for r in range(s.nr):
            m=None
            for c in range(s.nr): m=A(0,r,c,m)
        for t in range(len(st)):
            for r in range(s.nr):
                m=cx=None
                for c in range(s.nr):
                    if t+1<len(st): m=A(t+1,r,c,m)
                    cx=B(t,r,c,cx)
        for sel,i in ((0,y),(1,s.ns-1-y)):
            l=ls[sel]
            oT[:,s.at(i)]=(acc[sel]*(1.0/l)).astype(bf16)
            lse[i]=ms[sel]+jnp.log2(l)
    def backward(s, y, q, do, qT, doT, kT, vT, oT, lse, lsc, dsc, dqT, dkT, dvT, bufs):
        for sel,i in ((0,y),(1,s.ns-1-y)):
            drow=jnp.sum(doT[:,s.at(i)].astype(f32)*oT[:,s.at(i)].astype(f32),axis=0,keepdims=True)
            lsc[sel]=jnp.broadcast_to(lse[i],(128,s.seg)).T
            dsc[sel]=jnp.broadcast_to(drow,(128,s.seg)).T
        st=s.steps(y)
        def A(t,r): sel,qi,ki,dg=st[t]; s.ba(q,do,kT,vT,lsc,dsc,bufs[t%2],qi,sel,ki,dg,r)
        def B(t,r,cx): sel,qi,ki,dg=st[t]; return s.bb(qT,doT,kT,dqT,dkT,dvT,bufs[t%2],qi,sel,ki,dg,r,cx)
        for r in range(s.nr): A(0,r)
        for t in range(len(st)):
            cx=None
            for r in range(s.nr):
                if t+1<len(st): A(t+1,r)
                cx=B(t,r,cx)


MESH = pl.DeviceIdType.MESH


def kernel(n, qh, doh, kh, vh, oo, dqo, dko, dvo, q, do, ob, k, v, kT, vT, qT, doT, oT, lse, acc, ms, ls, lsc, dsc, dqT, dkT, dvT,
           s0, s1, m0, m1, p0, p1, d0, d1, t0, t1, insem, outsem, rk, rv, rq, rdo, ro, rdq, rdk, rdv):
    heads, shard, dim = qh.shape[1:]
    half = shard // 2
    segs = n
    core = Core(shard, segs, dim)
    me = lax.axis_index("ctx")
    scale = dim ** -0.5

    barrier = pltpu.get_barrier_semaphore()
    for off in range(1, n):
        pl.semaphore_signal(barrier, inc=1, device_id={"ctx": lax.rem(me + off, n)}, device_id_type=MESH)
    pl.semaphore_wait(barrier, n - 1)

    def rows(piece):
        return pl.ds(pl.multiple_of(piece * half, half), half)

    def own(part):
        return pl.ds(part * half, half)

    def piece(dev, part):
        return dev if part == 0 else 2 * n - 1 - dev

    def spread(src, dst, sem):
        for part in (0, 1):
            pltpu.make_async_copy(src(me, part), dst(part), sem).start()

        def send(off, _):
            dev = lax.rem(me + off, n)
            for part in (0, 1):
                pltpu.make_async_remote_copy(src(dev, part), dst(part), insem.at[dev], sem, device_id={"ctx": dev}, device_id_type=MESH).start()
            return 0

        lax.fori_loop(1, n, send, 0)

    def gather(src, dst, sem):
        for part in (0, 1):
            pltpu.make_async_copy(src(me, part), dst(part), sem).start()

        def send(off, _):
            dev = lax.rem(me + off, n)
            for part in (0, 1):
                pltpu.make_async_remote_copy(src(dev, part), dst(part), outsem.at[dev], sem, device_id={"ctx": dev}, device_id_type=MESH).start()
            return 0

        lax.fori_loop(1, n, send, 0)

    def arrived(ref, sem):
        pltpu.make_async_remote_copy(ref, ref, insem.at[me], sem, device_id={"ctx": lax.rem(me + 1, n)}, device_id_type=MESH).wait_recv()

    def sent(sem):
        pltpu.make_async_remote_copy(kh, kh, sem, rk, device_id={"ctx": lax.rem(me + 1, n)}, device_id_type=MESH).wait_send()

    spread(lambda dev, part: kh.at[dev, own(part)], lambda part: k.at[rows(piece(me, part))], rk)
    spread(lambda dev, part: vh.at[dev, own(part)], lambda part: v.at[rows(piece(me, part))], rv)
    for h in range(heads):
        spread(lambda dev, part: qh.at[dev, h, own(part)], lambda part: q.at[h, rows(piece(me, part))], rq.at[h])
        spread(lambda dev, part: doh.at[dev, h, own(part)], lambda part: do.at[h, rows(piece(me, part))], rdo.at[h])

    def turn(src, dst):
        def body(i, _):
            dst[:, core.at(i)] = src[core.at(i), :].T
            return 0

        lax.fori_loop(0, segs, body, 0)

    dkT[...] = jnp.zeros_like(dkT)
    dvT[...] = jnp.zeros_like(dvT)
    arrived(k, rk)
    turn(k, kT)
    arrived(v, rv)
    turn(v, vT)

    def head(h, _):
        arrived(q.at[h], rq.at[h])
        turn(q.at[h], qT)

        def fwd(y, _):
            core.forward(y, k, vT, qT, oT, lse, (s0, s1), (m0, m1), acc, ms, ls)
            for i in (y, segs - 1 - y):
                ob[h, core.at(i), :] = oT[:, core.at(i)].T
            return 0

        lax.fori_loop(0, segs // 2, fwd, 0)
        arrived(do.at[h], rdo.at[h])
        turn(do.at[h], doT)
        gather(lambda dev, part: ob.at[h, rows(piece(dev, part))], lambda part: oo.at[me, h, own(part)], ro)

        def bwd(y, _):
            core.backward(y, q.at[h], do.at[h], qT, doT, kT, vT, oT, lse, lsc, dsc, dqT, dkT, dvT, ((p0, d0, t0), (p1, d1, t1)))
            for sel, i in ((0, y), (1, segs - 1 - y)):
                q[h, core.at(i), :] = (dqT[sel] * scale).astype(bf16).T
            return 0

        lax.fori_loop(0, segs // 2, bwd, 0)
        gather(lambda dev, part: q.at[h, rows(piece(dev, part))], lambda part: dqo.at[me, h, own(part)], rdq)
        return 0

    lax.fori_loop(0, heads, head, 0)

    def finish(i, _):
        k[core.at(i), :] = (dkT[:, core.at(i)] * scale).astype(bf16).T
        v[core.at(i), :] = dvT[:, core.at(i)].astype(bf16).T
        return 0

    lax.fori_loop(0, segs, finish, 0)
    gather(lambda dev, part: k.at[rows(piece(dev, part))], lambda part: dko.at[me, own(part)], rdk)
    gather(lambda dev, part: v.at[rows(piece(dev, part))], lambda part: dvo.at[me, own(part)], rdv)
    for off in range(1, n):
        sent(insem.at[lax.rem(me + off, n)])
        sent(outsem.at[lax.rem(me + off, n)])
    arrived(oo, ro)
    arrived(dqo, rdq)
    arrived(dko, rdk)
    arrived(dvo, rdv)


def solution(mesh):
    n = mesh.shape["ctx"]
    spec = P("data", "ctx", None, None)

    def local(queries, keys_in, values_in, grad_out):
        batch, shard, heads, dim = queries.shape
        assert batch == n and keys_in.shape[2] == 1
        seq = n * shard
        q, g = (t.transpose(0, 2, 1, 3) for t in (queries, grad_out))
        k, v = (t.reshape(batch, shard, dim) for t in (keys_in, values_in))
        hbm = pl.BlockSpec(memory_space=pl.ANY)
        vm, dma = pltpu.VMEM, pltpu.SemaphoreType.DMA
        wide = jax.ShapeDtypeStruct(q.shape, bf16)
        thin = jax.ShapeDtypeStruct(k.shape, bf16)
        o, dq, dk, dv = pl.pallas_call(
            functools.partial(kernel, n),
            out_shape=[wide, wide, thin, thin],
            in_specs=[hbm] * 4,
            out_specs=[hbm] * 4,
            scratch_shapes=[vm((heads, seq, dim), bf16)] * 3 + [vm((seq, dim), bf16)] * 2 + [vm((dim, seq), bf16)] * 5
            + [vm((n, 1, shard), f32), vm((2, dim, shard), f32), vm((2, 1, shard), f32), vm((2, 1, shard), f32)]
            + [vm((2, shard, 128), f32)] * 2 + [vm((2, dim, shard), f32)] + [vm((dim, seq), f32)] * 2
            + [vm((shard, shard), f32)] * 2 + [vm((1, shard), f32)] * 2 + [vm((shard, shard), bf16)] * 6
            + [dma((n,)), dma((n,)), dma, dma, dma((heads,)), dma((heads,)), dma, dma, dma, dma],
            compiler_params=pltpu.CompilerParams(collective_id=0, has_side_effects=True, vmem_limit_bytes=67043328),
            name="attention",
        )(q, g, k, v)
        o, dq = (t.transpose(0, 2, 1, 3) for t in (o, dq))
        dk, dv = (t.reshape(keys_in.shape) for t in (dk, dv))
        return o, dq, dk, dv

    return jax.shard_map(local, mesh=mesh, in_specs=(spec,) * 4, out_specs=(spec,) * 4, check_vma=False)
```

```python
import functools
import math

import jax
import jax.numpy as jnp
from jax import lax
from jax.experimental import pallas as pl
from jax.experimental.pallas import tpu as pltpu
from jax.sharding import PartitionSpec as P

MESH = pl.DeviceIdType.MESH
f32, bf16 = jnp.float32, jnp.bfloat16
NEG = -1e30
R = 256


def dot(a, b):
    return jnp.dot(a, b, preferred_element_type=f32)


def triangle(flip):
    i, j = lax.broadcasted_iota(jnp.int32, (R, R), 0), lax.broadcasted_iota(jnp.int32, (R, R), 1)
    return i <= j if flip else i >= j


def kernel(n, qh, doh, kh, vh, oo, dqo, dko, dvo, q, do, ob, k, v, kT, vT, qT, doT, oT, acc, ms, ls, lsc, dsc, dkT, dvT,
           sb0, sb1, sb2, mb0, mb1, mb2, pb0, pb1, pb2, db0, db1, db2, tb0, tb1, tb2, insem, outsem, rk, rv, rq, rdo, ro, rdq, rdk, rdv):
    heads, shard, dim = qh.shape[1:]
    half, seg, segs, chips = shard // 2, shard, n, n // 2
    nr = seg // R
    sbs, mbs, bufs = (sb0, sb1, sb2), (mb0, mb1, mb2), ((pb0, db0, tb0), (pb1, db1, tb1), (pb2, db2, tb2))
    me = lax.axis_index("ctx")
    chip = me // 2
    scale = dim ** -0.5
    c2 = scale * math.log2(math.e)

    barrier = pltpu.get_barrier_semaphore()
    for off in range(1, n):
        pl.semaphore_signal(barrier, inc=1, device_id={"ctx": lax.rem(me + off, n)}, device_id_type=MESH)
    pl.semaphore_wait(barrier, n - 1)

    def rows(piece):
        return pl.ds(pl.multiple_of(piece * half, half), half)

    def at(i, r=None, m=1):
        if r is None:
            return pl.ds(pl.multiple_of(i * seg, seg), seg)
        return pl.ds(pl.multiple_of(i * seg + r * R, R), m * R)

    def to(dev, src, dst, sends, recvs):
        pltpu.make_async_remote_copy(src, dst, sends.at[dev], recvs, device_id={"ctx": dev}, device_id_type=MESH).start()

    def arrived(ref, sem):
        pltpu.make_async_remote_copy(ref, ref, insem.at[me], sem, device_id={"ctx": lax.rem(me + 1, n)}, device_id_type=MESH).wait_recv()

    def sent(sem):
        pltpu.make_async_remote_copy(kh, kh, sem, rdk, device_id={"ctx": lax.rem(me + 1, n)}, device_id_type=MESH).wait_send()

    pairs = [(kh, k, rk), (vh, v, rv), (qh, q, rq), (doh, do, rdo)]

    def part(which, dev, p):
        src, dst, _ = pairs[which]
        place = rows(me if p == 0 else 2 * n - 1 - me)
        own = pl.ds(p * half, half)
        return (src.at[dev, own], dst.at[place]) if which < 2 else (src.at[dev, :, own], dst.at[:, place])

    def give(which, dev, rel):
        for p in (0, 1):
            to(dev, *part(which, dev, p), insem, pairs[which][2].at[rel])

    other = me + 1 - 2 * lax.rem(me, 2)
    for which in range(4):
        for p in (0, 1):
            pltpu.make_async_copy(*part(which, me, p), pairs[which][2].at[0]).start()
        give(which, other, 0)
    for group, hops in (((0, 1), (1, 3, 2)), ((2, 3), (1, 3)), ((2, 3), (2,))):
        for which in group:
            for hop in hops:
                for core in (0, 1):
                    give(which, lax.rem(chip + hop, chips) * 2 + core, (chips - hop) % chips)

    def hand(ref, place, piece, sem):
        early = piece < n
        dev = jnp.where(early, piece, 2 * n - 1 - piece)
        own = pl.ds(pl.multiple_of(jnp.where(early, 0, half), half), half)
        src, dst = ref.at[rows(piece)], place.at[own]

        @pl.when(dev == me)
        def _():
            pltpu.make_async_copy(src, dst, sem).start()

        @pl.when(dev != me)
        def _():
            to(dev, src, dst, outsem, sem)

    def turn(src, dst, i, j):
        dst[:, at(j)] = src[at(i), :].T

    def phase(y, j, first, second, own, before, after):
        a, b = y, segs - 1 - y
        z = jnp.minimum(j, 0) * R
        diag = [(0, a, a), (1, b, b)]

        def full(t):
            if own:
                late = jnp.logical_or(t < 1, t > y)
                i = t - y - 1
                key = jnp.where(t < 1, a, jnp.where(late, jnp.where(i < a, i, i + 1), t - 1))
                return jnp.where(late, 1, 0), jnp.where(late, b, a), key
            early = t < y
            return jnp.where(early, 0, 1), jnp.where(early, a, b), jnp.where(early, t, t - y)

        def both(nxt, cur, z):
            carry = {}
            for r in range(nr):
                if nxt is not None:
                    first(*nxt, r, z)
                second(*cur, r, z, carry)

        for r in range(nr):
            first(True, diag[0], 0, r, z)
        order = [(True, d, h) for d in diag for h in range(heads)] + [(False, full(0), 0)]
        for cur, nxt in zip(order, order[1:]):
            both(nxt, cur, z)
        before()

        def loop(t, _):
            z = jnp.minimum(t, 0) * R
            now, later = full(t), full(t + 1)
            for h in range(heads):
                both((False, now, h + 1) if h + 1 < heads else (False, later, 0), (False, now, h), z)
            after(t)
            return 0

        lax.fori_loop(0, segs - 2, loop, 0)
        now = full(segs - 2)
        for h in range(heads):
            both((False, now, h + 1) if h + 1 < heads else None, (False, now, h), z)
        after(segs - 2)

    def span(z, c):
        return pl.ds(pl.multiple_of(z + c * R, R), R)

    def cols(sel, r):
        return pl.ds(pl.multiple_of(sel * seg + r * R, R), R)

    def fwd_a(diag, step, h, r, z):
        sel, qi, ki = step
        cs = slice(r * R, (r + 1) * R)
        m = None
        for c in range(r + 1 if diag else nr):
            x = dot(k[at(ki, c), :], qT[h, :, cols(sel, r)])
            if diag and c == r:
                x = jnp.where(triangle(True), x, NEG)
            sbs[h][span(z, c), cs] = x
            x = jnp.max(x, axis=0, keepdims=True)
            m = x if m is None else jnp.maximum(m, x)
        mbs[h][:, cs] = m

    def fwd_b(diag, step, h, r, z, carry):
        sel, qi, ki = step
        e = 2 * h + sel
        cs = slice(r * R, (r + 1) * R)
        m = mbs[h][:, cs] * c2
        if not diag:
            m = jnp.maximum(ms[e, :, cs], m)
        l = o = None
        for c in range(r + 1 if diag else nr):
            p = jnp.exp2(sbs[h][span(z, c), cs] * c2 - m)
            x, w = jnp.sum(p, axis=0, keepdims=True), dot(vT[:, at(ki, c)], p.astype(bf16))
            l, o = (x, w) if l is None else (l + x, o + w)
        if not diag:
            fade = jnp.exp2(ms[e, :, cs] - m)
            l = l + ls[e, :, cs] * fade
            o = o + acc[e, :, cs] * fade
        ms[e, :, cs] = m
        ls[e, :, cs] = l
        acc[e, :, cs] = o

    def bwd_a(diag, step, h, r, z):
        sel, qi, ki = step
        e = 2 * h + sel
        pb, db, tb = bufs[h]
        m = r + 1 if diag else nr
        w = m * R
        rs = slice(r * R, (r + 1) * R)
        s = dot(q[h, at(qi, r), :], kT[:, at(ki, 0, m)])
        dp = dot(do[h, at(qi, r), :], vT[:, at(ki, 0, m)])
        l = jnp.concatenate([lsc[e, rs, :]] * (w // 128), axis=1)
        d = jnp.concatenate([dsc[e, rs, :]] * (w // 128), axis=1)
        p = jnp.exp2(s * c2 - l)
        if diag:
            t = jnp.where(triangle(False), p[:, r * R:], 0.0)
            p = jnp.concatenate([p[:, :r * R], t], axis=1) if r else t
        ds = (p * (dp - d)).astype(bf16)
        pb[rs, :w] = p.astype(bf16)
        db[rs, :w] = ds
        tb[:w, rs] = ds.T

    def bwd_b(diag, step, h, r, z, carry):
        sel, qi, ki = step
        e = 2 * h + sel
        pb, db, tb = bufs[h]
        m = r + 1 if diag else nr
        w = m * R
        rs = slice(r * R, (r + 1) * R)
        ks = at(ki, 0, m)
        x = dot(doT[h, :, cols(sel, r)], pb[rs, :w])
        g = dot(qT[h, :, cols(sel, r)], db[rs, :w])
        u = dot(kT[:, ks], tb[:w, rs])
        if diag:
            acc[e, :, rs] = u
            dvT[:, ks] += x
            dkT[:, ks] += g
            return
        acc[e, :, rs] += u
        if r:
            x, g = carry["v"] + x, carry["k"] + g
        carry["v"], carry["k"] = x, g
        if r == nr - 1:
            dvT[:, ks] += x
            dkT[:, ks] += g

    def give_keys(i):
        k[at(i), :] = (dkT[:, at(i)] * scale).astype(bf16).T
        v[at(i), :] = dvT[:, at(i)].astype(bf16).T
        for p in (0, 1):
            hand(k, dko.at[me], 2 * i + p, rdk)
            hand(v, dvo.at[me], 2 * i + p, rdv)

    def give_queries(sel, i):
        for h in range(heads):
            q[h, at(i), :] = (acc[2 * h + sel] * scale).astype(bf16).T
        for h in range(heads):
            for p in (0, 1):
                hand(q.at[h], dqo.at[me, h], 2 * i + p, rdq)

    def set_of(j, _):
        rel = jnp.where(j == 2, 3, jnp.where(j == 3, 2, j))
        y = lax.rem(chip + rel, chips)
        a, b = y, segs - 1 - y
        last = j == chips - 1
        both = ((0, a), (1, b))

        def keys(r, ref, sem, out):
            arrived(ref.at[pl.ds(0, 2 * seg)], sem.at[r])
            x = lax.rem(chip + r, chips)
            for i in (x, segs - 1 - x):
                turn(ref, out, i, i)

        @pl.when(j == 0)
        def _():
            keys(0, k, rk, kT)
            keys(0, v, rv, vT)

        arrived(q.at[:, pl.ds(0, 2 * seg)], rq.at[rel])
        for h in range(heads):
            for sel, i in both:
                turn(q.at[h], qT.at[h], i, sel)

        def rest():
            @pl.when(j == 0)
            def _():
                for ref, sem, out in ((k, rk, kT), (v, rv, vT)):
                    def one(r, _):
                        keys(r, ref, sem, out)
                        return 0
                    lax.fori_loop(1, chips, one, 0)

        phase(y, j, fwd_a, fwd_b, True, rest, lambda t: None)
        for sel, i in both:
            for h in range(heads):
                e = 2 * h + sel
                l = ls[e]
                o = (acc[e] * (1.0 / l)).astype(bf16)
                oT[h, :, at(sel)] = o
                ob[h, at(i), :] = o.T
                lsc[e] = jnp.broadcast_to(ms[e] + jnp.log2(l), (128, seg)).T
        for sel, i in both:
            for h in range(heads):
                for p in (0, 1):
                    hand(ob.at[h], oo.at[me, h], 2 * i + p, ro)
        arrived(do.at[:, pl.ds(0, 2 * seg)], rdo.at[rel])
        for h in range(heads):
            for sel, i in both:
                g = do[h, at(i), :].T
                doT[h, :, at(sel)] = g
                d = jnp.sum(g.astype(f32) * oT[h, :, at(sel)].astype(f32), axis=0, keepdims=True)
                dsc[2 * h + sel] = jnp.broadcast_to(d, (128, seg)).T

        def ready():
            @pl.when(last)
            def _():
                def one(i, _):
                    give_keys(i)
                    return 0
                lax.fori_loop(b, segs, one, 0)

        def done(t):
            @pl.when(jnp.logical_and(last, t >= y))
            def _():
                give_keys(t - y)

            @pl.when(t == y)
            def _():
                give_queries(0, a)

        phase(y, j, bwd_a, bwd_b, False, ready, done)
        give_queries(1, b)
        return 0

    dkT[...] = jnp.zeros_like(dkT)
    dvT[...] = jnp.zeros_like(dvT)
    lax.fori_loop(0, chips, set_of, 0)
    for off in range(1, n):
        sent(insem.at[lax.rem(me + off, n)])
        sent(outsem.at[lax.rem(me + off, n)])
    arrived(oo, ro)
    arrived(dqo, rdq)
    arrived(dko, rdk)
    arrived(dvo, rdv)


def solution(mesh):
    n = mesh.shape["ctx"]
    spec = P("data", "ctx", None, None)

    def local(queries, keys_in, values_in, grad_out):
        batch, shard, heads, dim = queries.shape
        assert batch == n and keys_in.shape[2] == 1
        seq = n * shard
        q, g = (t.transpose(0, 2, 1, 3) for t in (queries, grad_out))
        k, v = (t.reshape(batch, shard, dim) for t in (keys_in, values_in))
        hbm = pl.BlockSpec(memory_space=pl.ANY)
        vm, dma = pltpu.VMEM, pltpu.SemaphoreType.DMA
        wide = jax.ShapeDtypeStruct(q.shape, bf16)
        thin = jax.ShapeDtypeStruct(k.shape, bf16)
        o, dq, dk, dv = pl.pallas_call(
            functools.partial(kernel, n),
            out_shape=[wide, wide, thin, thin],
            in_specs=[hbm] * 4,
            out_specs=[hbm] * 4,
            scratch_shapes=[vm((heads, seq, dim), bf16)] * 3 + [vm((seq, dim), bf16)] * 2 + [vm((dim, seq), bf16)] * 2
            + [vm((heads, dim, 2 * shard), bf16)] * 3
            + [vm((2 * heads, dim, shard), f32), vm((2 * heads, 1, shard), f32), vm((2 * heads, 1, shard), f32)]
            + [vm((2 * heads, shard, 128), f32)] * 2 + [vm((dim, seq), f32)] * 2
            + [vm((shard, shard), f32)] * 3 + [vm((1, shard), f32)] * 3 + [vm((shard, shard), bf16)] * 9
            + [dma((n,)), dma((n,))] + [dma((n // 2,))] * 4 + [dma] * 4,
            compiler_params=pltpu.CompilerParams(collective_id=0, has_side_effects=True, vmem_limit_bytes=67043328),
            name="attention",
        )(q, g, k, v)
        o, dq = (t.transpose(0, 2, 1, 3) for t in (o, dq))
        dk, dv = (t.reshape(keys_in.shape) for t in (dk, dv))
        return o, dq, dk, dv

    return jax.shard_map(local, mesh=mesh, in_specs=(spec,) * 4, out_specs=(spec,) * 4, check_vma=False)
```

```python
import functools
import math

import jax
import jax.numpy as jnp
from jax import lax
from jax.experimental import pallas as pl
from jax.experimental.pallas import tpu as pltpu
from jax.sharding import PartitionSpec as P

MESH = pl.DeviceIdType.MESH
f32, bf16 = jnp.float32, jnp.bfloat16
NEG = -1e30
R = 256


def dot(a, b):
    return jnp.dot(a, b, preferred_element_type=f32)


def triangle(flip):
    i, j = lax.broadcasted_iota(jnp.int32, (R, R), 0), lax.broadcasted_iota(jnp.int32, (R, R), 1)
    return i <= j if flip else i >= j


def kernel(n, qh, doh, kh, vh, oo, dqo, dko, dvo, q, do, ob, k, v, kT, vT, qT, doT, acc, ms, ls, lse, lsc, dsc, dkT, dvT,
           sb0, sb1, sb2, mb0, mb1, mb2, pb0, pb1, pb2, db0, db1, db2, tb0, tb1, tb2, insem, outsem, rk, rv, rq, rdo, ro, rdq, rdk, rdv):
    heads, shard, dim = qh.shape[1:]
    half, seg, segs, chips = shard // 2, shard, n, n // 2
    nr = seg // R
    sbs, mbs, bufs = (sb0, sb1, sb2), (mb0, mb1, mb2), ((pb0, db0, tb0), (pb1, db1, tb1), (pb2, db2, tb2))
    me = lax.axis_index("ctx")
    chip = me // 2
    scale = dim ** -0.5
    c2 = scale * math.log2(math.e)

    barrier = pltpu.get_barrier_semaphore()
    for off in range(1, n):
        pl.semaphore_signal(barrier, inc=1, device_id={"ctx": lax.rem(me + off, n)}, device_id_type=MESH)
    pl.semaphore_wait(barrier, n - 1)

    def rows(piece):
        return pl.ds(pl.multiple_of(piece * half, half), half)

    def at(i, r=None, m=1):
        if r is None:
            return pl.ds(pl.multiple_of(i * seg, seg), seg)
        return pl.ds(pl.multiple_of(i * seg + r * R, R), m * R)

    def to(dev, src, dst, sends, recvs):
        pltpu.make_async_remote_copy(src, dst, sends.at[dev], recvs, device_id={"ctx": dev}, device_id_type=MESH).start()

    def arrived(ref, sem):
        pltpu.make_async_remote_copy(ref, ref, insem.at[me], sem, device_id={"ctx": lax.rem(me + 1, n)}, device_id_type=MESH).wait_recv()

    def sent(sem):
        pltpu.make_async_remote_copy(kh, kh, sem, rdk, device_id={"ctx": lax.rem(me + 1, n)}, device_id_type=MESH).wait_send()

    pairs = [(kh, k, rk), (vh, v, rv), (qh, q, rq), (doh, do, rdo)]

    def part(which, dev, p):
        src, dst, _ = pairs[which]
        place = rows(me if p == 0 else 2 * n - 1 - me)
        own = pl.ds(p * half, half)
        return (src.at[dev, own], dst.at[place]) if which < 2 else (src.at[dev, :, own], dst.at[:, place])

    def landing(which, rel, p):
        return pairs[which][2].at[p * chips + rel] if which < 2 else pairs[which][2].at[rel]

    def give(which, dev, rel, halves=(0, 1)):
        for p in halves:
            to(dev, *part(which, dev, p), insem, landing(which, rel, p))

    other = me + 1 - 2 * lax.rem(me, 2)
    for which in range(4):
        for p in (0, 1):
            pltpu.make_async_copy(*part(which, me, p), landing(which, 0, p)).start()
        give(which, other, 0)
    for group, hops, halves in (((0, 1), (1, 3, 2), (0,)), ((0, 1), (1, 3, 2), (1,)), ((2, 3), (1, 3), (0, 1)), ((2, 3), (2,), (0, 1))):
        for which in group:
            for hop in hops:
                for core in (0, 1):
                    give(which, lax.rem(chip + hop, chips) * 2 + core, (chips - hop) % chips, halves)

    def hand(ref, place, piece, sem):
        early = piece < n
        dev = jnp.where(early, piece, 2 * n - 1 - piece)
        own = pl.ds(pl.multiple_of(jnp.where(early, 0, half), half), half)
        src, dst = ref.at[rows(piece)], place.at[own]

        @pl.when(dev == me)
        def _():
            pltpu.make_async_copy(src, dst, sem).start()

        @pl.when(dev != me)
        def _():
            to(dev, src, dst, outsem, sem)

    def turn(src, dst, i, j):
        dst[:, at(j)] = src[at(i), :].T

    def phase(y, j, first, second, own, before, after):
        a, b = y, segs - 1 - y
        z = jnp.minimum(j, 0) * R
        diag = [(0, a, a), (1, b, b)]

        def full(t):
            if own:
                late = jnp.logical_or(t < 1, t > y)
                i = t - y - 1
                key = jnp.where(t < 1, a, jnp.where(late, jnp.where(i < a, i, i + 1), t - 1))
                return jnp.where(late, 1, 0), jnp.where(late, b, a), key
            early = t < y
            return jnp.where(early, 0, 1), jnp.where(early, a, b), jnp.where(early, t, t - y)

        def both(nxt, cur, z):
            carry = {}
            for r in range(nr):
                if nxt is not None:
                    first(*nxt, r, z)
                second(*cur, r, z, carry)

        for r in range(nr):
            first(True, diag[0], 0, r, z)
        order = [(True, d, h) for d in diag for h in range(heads)] + [(False, full(0), 0)]
        for cur, nxt in zip(order, order[1:]):
            both(nxt, cur, z)
        before()

        def loop(t, _):
            z = jnp.minimum(t, 0) * R
            now, later = full(t), full(t + 1)
            for h in range(heads):
                both((False, now, h + 1) if h + 1 < heads else (False, later, 0), (False, now, h), z)

        def two(i, _):
            loop(2 * i, 0)
            loop(2 * i + 1, 0)
            after(2 * i)
            return 0

        lax.fori_loop(0, (segs - 2) // 2, two, 0)
        now = full(segs - 2)
        for h in range(heads):
            both((False, now, h + 1) if h + 1 < heads else None, (False, now, h), z)
        after(segs - 2)

    def span(z, c):
        return pl.ds(pl.multiple_of(z + c * R, R), R)

    def cols(sel, r):
        return pl.ds(pl.multiple_of(sel * seg + r * R, R), R)

    def fwd_a(diag, step, h, r, z):
        sel, qi, ki = step
        cs = slice(r * R, (r + 1) * R)
        m = None
        for c in range(r + 1 if diag else nr):
            x = dot(k[at(ki, c), :], qT[h, :, cols(sel, r)])
            if diag and c == r:
                x = jnp.where(triangle(True), x, NEG)
            sbs[h][span(z, c), cs] = x
            x = jnp.max(x, axis=0, keepdims=True)
            m = x if m is None else jnp.maximum(m, x)
        mbs[h][:, cs] = m

    def fwd_b(diag, step, h, r, z, carry):
        sel, qi, ki = step
        e = 2 * h + sel
        cs = slice(r * R, (r + 1) * R)
        m = mbs[h][:, cs] * c2
        if not diag:
            m = jnp.maximum(ms[e, :, cs], m)
        l = o = None
        for c in range(r + 1 if diag else nr):
            p = jnp.exp2(sbs[h][span(z, c), cs] * c2 - m)
            x, w = jnp.sum(p, axis=0, keepdims=True), dot(vT[:, at(ki, c)], p.astype(bf16))
            l, o = (x, w) if l is None else (l + x, o + w)
        if not diag:
            fade = jnp.exp2(ms[e, :, cs] - m)
            l = l + ls[e, :, cs] * fade
            o = o + acc[e, :, cs] * fade
        ms[e, :, cs] = m
        ls[e, :, cs] = l
        acc[e, :, cs] = o

    def bwd_a(diag, step, h, r, z):
        sel, qi, ki = step
        e = 2 * h + sel
        pb, db, tb = bufs[h]
        m = r + 1 if diag else nr
        w = m * R
        rs = slice(r * R, (r + 1) * R)
        s = dot(q[h, at(qi, r), :], kT[:, at(ki, 0, m)])
        dp = dot(do[h, at(qi, r), :], vT[:, at(ki, 0, m)])
        l = jnp.concatenate([lsc[e, rs, :]] * (w // 128), axis=1)
        d = jnp.concatenate([dsc[e, rs, :]] * (w // 128), axis=1)
        p = jnp.exp2(s * c2 - l)
        if diag:
            t = jnp.where(triangle(False), p[:, r * R:], 0.0)
            p = jnp.concatenate([p[:, :r * R], t], axis=1) if r else t
        ds = (p * (dp - d)).astype(bf16)
        pb[rs, :w] = p.astype(bf16)
        db[rs, :w] = ds
        tb[:w, rs] = ds.T

    def bwd_b(diag, step, h, r, z, carry):
        sel, qi, ki = step
        e = 2 * h + sel
        pb, db, tb = bufs[h]
        m = r + 1 if diag else nr
        w = m * R
        rs = slice(r * R, (r + 1) * R)
        ks = at(ki, 0, m)
        x = dot(doT[h, :, cols(sel, r)], pb[rs, :w])
        g = dot(qT[h, :, cols(sel, r)], db[rs, :w])
        u = dot(kT[:, ks], tb[:w, rs])
        if diag:
            acc[e, :, rs] = u
            dvT[:, ks] += x
            dkT[:, ks] += g
            return
        acc[e, :, rs] += u
        if r:
            x, g = carry["v"] + x, carry["k"] + g
        carry["v"], carry["k"] = x, g
        if r == nr - 1:
            dvT[:, ks] += x
            dkT[:, ks] += g

    def give_keys(i):
        k[at(i), :] = (dkT[:, at(i)] * scale).astype(bf16).T
        v[at(i), :] = dvT[:, at(i)].astype(bf16).T
        for p in (0, 1):
            hand(k, dko.at[me], 2 * i + p, rdk)
            hand(v, dvo.at[me], 2 * i + p, rdv)

    def give_queries(sel, i):
        for h in range(heads):
            q[h, at(i), :] = (acc[2 * h + sel] * scale).astype(bf16).T
        for h in range(heads):
            for p in (0, 1):
                hand(q.at[h], dqo.at[me, h], 2 * i + p, rdq)

    def keys(rel, p):
        x = lax.rem(chip + rel, chips)
        i = x if p == 0 else segs - 1 - x
        for ref, sem, out in ((k, rk, kT), (v, rv, vT)):
            arrived(ref.at[pl.ds(0, seg)], sem.at[p * chips + rel])
            turn(ref, out, i, i)

    def others(p):
        def one(rel, _):
            keys(rel, p)
            return 0

        lax.fori_loop(1, chips, one, 0)

    def place(j):
        rel = jnp.where(j == 2, 3, jnp.where(j == 3, 2, j))
        y = lax.rem(chip + rel, chips)
        a, b = y, segs - 1 - y
        return rel, y, a, b, ((0, a), (1, b))

    def turn_queries(both):
        for h in range(heads):
            for sel, i in both:
                turn(q.at[h], qT.at[h], i, sel)

    def forward(j):
        rel, y, a, b, both = place(j)
        arrived(q.at[:, pl.ds(0, 2 * seg)], rq.at[rel])
        turn_queries(both)

        def low():
            @pl.when(j == 0)
            def _():
                others(0)

        def high(t):
            @pl.when(jnp.logical_and(j == 0, t == (y + 1) // 2 * 2))
            def _():
                others(1)

        phase(y, j, fwd_a, fwd_b, True, low, high)
        for sel, i in both:
            for h in range(heads):
                e = 2 * h + sel
                l = ls[e]
                ob[h, at(i), :] = (acc[e] * (1.0 / l)).astype(bf16).T
                lse[j, e] = ms[e] + jnp.log2(l)
        for sel, i in both:
            for h in range(heads):
                for p in (0, 1):
                    hand(ob.at[h], oo.at[me, h], 2 * i + p, ro)

    def backward(j, last):
        rel, y, a, b, both = place(j)
        arrived(do.at[:, pl.ds(0, 2 * seg)], rdo.at[rel])
        turn_queries(both)
        for h in range(heads):
            for sel, i in both:
                e = 2 * h + sel
                turn(do.at[h], doT.at[h], i, sel)
                lsc[e] = jnp.broadcast_to(lse[j, e], (128, seg)).T
                for r in range(nr):
                    d = jnp.sum(do[h, at(i, r), :].astype(f32) * ob[h, at(i, r), :].astype(f32), axis=1, keepdims=True)
                    dsc[e, r * R:(r + 1) * R, :] = jnp.broadcast_to(d, (R, 128))

        def ready():
            @pl.when(last)
            def _():
                def one(i, _):
                    give_keys(i)
                    return 0

                lax.fori_loop(b, segs, one, 0)

        def done(t):
            for i in (t, t + 1) if t is not segs - 2 else (t,):
                @pl.when(jnp.logical_and(last, i >= y))
                def _():
                    give_keys(i - y)

                @pl.when(i == y)
                def _():
                    give_queries(0, a)

        phase(y, j, bwd_a, bwd_b, False, ready, done)
        give_queries(1, b)

    def turns(s, _):
        is_f = jnp.logical_or(s < 3, s == 4)
        j = jnp.where(s < 3, s, jnp.where(s == 3, 1, jnp.where(s < 6, 3, jnp.where(s == 6, 2, 0))))

        @pl.when(is_f)
        def _():
            forward(j)

        @pl.when(jnp.logical_not(is_f))
        def _():
            backward(j, s == 7)

        return 0

    dkT[...] = jnp.zeros_like(dkT)
    dvT[...] = jnp.zeros_like(dvT)
    keys(0, 0)
    keys(0, 1)
    lax.fori_loop(0, 2 * chips, turns, 0)
    for off in range(1, n):
        sent(insem.at[lax.rem(me + off, n)])
        sent(outsem.at[lax.rem(me + off, n)])
    arrived(oo, ro)
    arrived(dqo, rdq)
    arrived(dko, rdk)
    arrived(dvo, rdv)


def solution(mesh):
    n = mesh.shape["ctx"]
    spec = P("data", "ctx", None, None)

    def local(queries, keys_in, values_in, grad_out):
        batch, shard, heads, dim = queries.shape
        assert batch == n and keys_in.shape[2] == 1
        seq = n * shard
        q, g = (t.transpose(0, 2, 1, 3) for t in (queries, grad_out))
        k, v = (t.reshape(batch, shard, dim) for t in (keys_in, values_in))
        hbm = pl.BlockSpec(memory_space=pl.ANY)
        vm, dma = pltpu.VMEM, pltpu.SemaphoreType.DMA
        wide = jax.ShapeDtypeStruct(q.shape, bf16)
        thin = jax.ShapeDtypeStruct(k.shape, bf16)
        o, dq, dk, dv = pl.pallas_call(
            functools.partial(kernel, n),
            out_shape=[wide, wide, thin, thin],
            in_specs=[hbm] * 4,
            out_specs=[hbm] * 4,
            scratch_shapes=[vm((heads, seq, dim), bf16)] * 3 + [vm((seq, dim), bf16)] * 2 + [vm((dim, seq), bf16)] * 2
            + [vm((heads, dim, 2 * shard), bf16)] * 2
            + [vm((2 * heads, dim, shard), f32), vm((2 * heads, 1, shard), f32), vm((2 * heads, 1, shard), f32), vm((n // 2, 2 * heads, 1, shard), f32)]
            + [vm((2 * heads, shard, 128), f32)] * 2 + [vm((dim, seq), f32)] * 2
            + [vm((shard, shard), f32)] * 3 + [vm((1, shard), f32)] * 3 + [vm((shard, shard), bf16)] * 9
            + [dma((n,)), dma((n,)), dma((n,)), dma((n,)), dma((n // 2,)), dma((n // 2,))] + [dma] * 4,
            compiler_params=pltpu.CompilerParams(collective_id=0, has_side_effects=True, vmem_limit_bytes=67043328),
            name="attention",
        )(q, g, k, v)
        o, dq = (t.transpose(0, 2, 1, 3) for t in (o, dq))
        dk, dv = (t.reshape(keys_in.shape) for t in (dk, dv))
        return o, dq, dk, dv

    return jax.shard_map(local, mesh=mesh, in_specs=(spec,) * 4, out_specs=(spec,) * 4, check_vma=False)
```

```python
import functools
import math

import jax
import jax.numpy as jnp
from jax import lax
from jax.experimental import pallas as pl
from jax.experimental.pallas import tpu as pltpu
from jax.sharding import PartitionSpec as P

MESH = pl.DeviceIdType.MESH
f32, bf16 = jnp.float32, jnp.bfloat16
NEG = -1e30
R = 256


def dot(a, b):
    return jnp.dot(a, b, preferred_element_type=f32)


def triangle(flip):
    i, j = lax.broadcasted_iota(jnp.int32, (R, R), 0), lax.broadcasted_iota(jnp.int32, (R, R), 1)
    return i <= j if flip else i >= j


def kernel(n, qh, doh, kh, vh, oo, dqo, dko, dvo, q, do, ob, k, v, kT, vT, qT, doT, acc, ms, ls, lse, lsc, dsc, dkT, dvT,
           sb0, sb1, mb0, mb1, pb0, pb1, db0, db1, tb0, tb1, insem, outsem, rk, rv, rq, rdo, ro, rdq, rdk, rdv):
    heads, shard, dim = qh.shape[1:]
    half, seg, segs, chips = shard // 2, shard, n, n // 2
    nr = seg // R
    sbs, mbs, bufs = (sb0, sb1), (mb0, mb1), ((pb0, db0, tb0), (pb1, db1, tb1))
    me = lax.axis_index("ctx")
    chip = me // 2
    scale = dim ** -0.5
    c2 = scale * math.log2(math.e)

    barrier = pltpu.get_barrier_semaphore()
    for off in range(1, n):
        pl.semaphore_signal(barrier, inc=1, device_id={"ctx": lax.rem(me + off, n)}, device_id_type=MESH)
    pl.semaphore_wait(barrier, n - 1)

    def rows(piece):
        return pl.ds(pl.multiple_of(piece * half, half), half)

    def at(i, r=None, m=1):
        if r is None:
            return pl.ds(pl.multiple_of(i * seg, seg), seg)
        return pl.ds(pl.multiple_of(i * seg + r * R, R), m * R)

    def to(dev, src, dst, sends, recvs):
        pltpu.make_async_remote_copy(src, dst, sends.at[dev], recvs, device_id={"ctx": dev}, device_id_type=MESH).start()

    def arrived(ref, sem):
        pltpu.make_async_remote_copy(ref, ref, insem.at[me], sem, device_id={"ctx": lax.rem(me + 1, n)}, device_id_type=MESH).wait_recv()

    def sent(sem):
        pltpu.make_async_remote_copy(kh, kh, sem, rdk, device_id={"ctx": lax.rem(me + 1, n)}, device_id_type=MESH).wait_send()

    pairs = [(kh, k, rk), (vh, v, rv), (qh, q, rq), (doh, do, rdo)]

    def part(which, dev, p):
        src, dst, _ = pairs[which]
        place = rows(me if p == 0 else 2 * n - 1 - me)
        own = pl.ds(p * half, half)
        return (src.at[dev, own], dst.at[place]) if which < 2 else (src.at[dev, :, own], dst.at[:, place])

    def landing(which, rel, p):
        return pairs[which][2].at[p * chips + rel] if which < 2 else pairs[which][2].at[rel]

    def give(which, dev, rel, halves=(0, 1)):
        for p in halves:
            to(dev, *part(which, dev, p), insem, landing(which, rel, p))

    other = me + 1 - 2 * lax.rem(me, 2)
    for which in range(4):
        for p in (0, 1):
            pltpu.make_async_copy(*part(which, me, p), landing(which, 0, p)).start()
        give(which, other, 0)
    for group, hops, halves in (((0, 1), (1, 3, 2), (0,)), ((0, 1), (1, 3, 2), (1,)), ((2, 3), (1, 3), (0, 1)), ((2, 3), (2,), (0, 1))):
        for which in group:
            for hop in hops:
                for core in (0, 1):
                    give(which, lax.rem(chip + hop, chips) * 2 + core, (chips - hop) % chips, halves)

    def hand(ref, place, piece, sem):
        early = piece < n
        dev = jnp.where(early, piece, 2 * n - 1 - piece)
        own = pl.ds(pl.multiple_of(jnp.where(early, 0, half), half), half)
        src, dst = ref.at[rows(piece)], place.at[own]

        @pl.when(dev == me)
        def _():
            pltpu.make_async_copy(src, dst, sem).start()

        @pl.when(dev != me)
        def _():
            to(dev, src, dst, outsem, sem)

    def turn(src, dst, i, j):
        dst[:, at(j)] = src[at(i), :].T

    def phase(y, j, first, second, own, before, after):
        a, b = y, segs - 1 - y
        z = jnp.minimum(j, 0) * R
        diag = [(0, a, a), (1, b, b)]

        def full(t):
            if own:
                late = jnp.logical_or(t < 1, t > y)
                i = t - y - 1
                key = jnp.where(t < 1, a, jnp.where(late, jnp.where(i < a, i, i + 1), t - 1))
                return jnp.where(late, 1, 0), jnp.where(late, b, a), key
            early = t < y
            return jnp.where(early, 0, 1), jnp.where(early, a, b), jnp.where(early, t, t - y)

        def both(nxt, cur, slot, z):
            carry = {}
            for r in range(nr):
                if nxt is not None:
                    first(*nxt, 1 - slot, r, z)
                second(*cur, slot, r, z, carry)

        for r in range(nr):
            first(True, diag[0], 0, 0, r, z)
        order = [(True, d, h) for d in diag for h in range(heads)] + [(False, full(0), 0)]
        for i, (cur, nxt) in enumerate(zip(order, order[1:])):
            both(nxt, cur, i % 2, z)
        before()

        def loop(t, odd):
            z = jnp.minimum(t, 0) * R
            now, later = full(t), full(t + 1)
            for h in range(heads):
                both((False, now, h + 1) if h + 1 < heads else (False, later, 0), (False, now, h), (2 * heads + heads * odd + h) % 2, z)

        def two(i, _):
            loop(2 * i, 0)
            loop(2 * i + 1, 1)
            after(2 * i)
            return 0

        lax.fori_loop(0, (segs - 2) // 2, two, 0)
        now = full(segs - 2)
        for h in range(heads):
            both((False, now, h + 1) if h + 1 < heads else None, (False, now, h), (2 * heads + heads * (segs - 2) + h) % 2, z)
        after(segs - 2)

    def span(z, c):
        return pl.ds(pl.multiple_of(z + c * R, R), R)

    def cols(sel, r):
        return pl.ds(pl.multiple_of(sel * seg + r * R, R), R)

    def fwd_a(diag, step, h, slot, r, z):
        sel, qi, ki = step
        cs = slice(r * R, (r + 1) * R)
        m = None
        for c in range(r + 1 if diag else nr):
            x = dot(k[at(ki, c), :], qT[h, :, cols(sel, r)])
            if diag and c == r:
                x = jnp.where(triangle(True), x, NEG)
            sbs[slot][span(z, c), cs] = x
            x = jnp.max(x, axis=0, keepdims=True)
            m = x if m is None else jnp.maximum(m, x)
        mbs[slot][:, cs] = m

    def fwd_b(diag, step, h, slot, r, z, carry):
        sel, qi, ki = step
        e = 2 * h + sel
        cs = slice(r * R, (r + 1) * R)
        m = mbs[slot][:, cs] * c2
        if not diag:
            m = jnp.maximum(ms[e, :, cs], m)
        l = o = None
        for c in range(r + 1 if diag else nr):
            p = jnp.exp2(sbs[slot][span(z, c), cs] * c2 - m)
            x, w = jnp.sum(p, axis=0, keepdims=True), dot(vT[:, at(ki, c)], p.astype(bf16))
            l, o = (x, w) if l is None else (l + x, o + w)
        if not diag:
            fade = jnp.exp2(ms[e, :, cs] - m)
            l = l + ls[e, :, cs] * fade
            o = o + acc[e, :, cs] * fade
        ms[e, :, cs] = m
        ls[e, :, cs] = l
        acc[e, :, cs] = o

    def bwd_a(diag, step, h, slot, r, z):
        sel, qi, ki = step
        e = 2 * h + sel
        pb, db, tb = bufs[slot]
        m = r + 1 if diag else nr
        w = m * R
        rs = slice(r * R, (r + 1) * R)
        s = dot(q[h, at(qi, r), :], kT[:, at(ki, 0, m)])
        dp = dot(do[h, at(qi, r), :], vT[:, at(ki, 0, m)])
        l = jnp.concatenate([lsc[e, rs, :]] * (w // 128), axis=1)
        d = jnp.concatenate([dsc[e, rs, :]] * (w // 128), axis=1)
        p = jnp.exp2(s * c2 - l)
        if diag:
            t = jnp.where(triangle(False), p[:, r * R:], 0.0)
            p = jnp.concatenate([p[:, :r * R], t], axis=1) if r else t
        ds = (p * (dp - d)).astype(bf16)
        pb[rs, :w] = p.astype(bf16)
        db[rs, :w] = ds
        tb[:w, rs] = ds.T

    def bwd_b(diag, step, h, slot, r, z, carry):
        sel, qi, ki = step
        e = 2 * h + sel
        pb, db, tb = bufs[slot]
        m = r + 1 if diag else nr
        w = m * R
        rs = slice(r * R, (r + 1) * R)
        ks = at(ki, 0, m)
        x = dot(doT[h, :, cols(sel, r)], pb[rs, :w])
        g = dot(qT[h, :, cols(sel, r)], db[rs, :w])
        u = dot(kT[:, ks], tb[:w, rs])
        if diag:
            acc[e, :, rs] = u
            dvT[:, ks] += x
            dkT[:, ks] += g
            return
        acc[e, :, rs] += u
        if r:
            x, g = carry["v"] + x, carry["k"] + g
        carry["v"], carry["k"] = x, g
        if r == nr - 1:
            dvT[:, ks] += x
            dkT[:, ks] += g

    def give_keys(i):
        k[at(i), :] = (dkT[:, at(i)] * scale).astype(bf16).T
        v[at(i), :] = dvT[:, at(i)].astype(bf16).T
        for p in (0, 1):
            hand(k, dko.at[me], 2 * i + p, rdk)
            hand(v, dvo.at[me], 2 * i + p, rdv)

    def give_queries(sel, i):
        for h in range(heads):
            q[h, at(i), :] = (acc[2 * h + sel] * scale).astype(bf16).T
        for h in range(heads):
            for p in (0, 1):
                hand(q.at[h], dqo.at[me, h], 2 * i + p, rdq)

    def keys(rel, p):
        x = lax.rem(chip + rel, chips)
        i = x if p == 0 else segs - 1 - x
        for ref, sem, out in ((k, rk, kT), (v, rv, vT)):
            arrived(ref.at[pl.ds(0, seg)], sem.at[p * chips + rel])
            turn(ref, out, i, i)

    def others(p):
        def one(rel, _):
            keys(rel, p)
            return 0

        lax.fori_loop(1, chips, one, 0)

    def place(j):
        rel = jnp.where(j == 2, 3, jnp.where(j == 3, 2, j))
        y = lax.rem(chip + rel, chips)
        a, b = y, segs - 1 - y
        return rel, y, a, b, ((0, a), (1, b))

    def turn_queries(both):
        for h in range(heads):
            for sel, i in both:
                turn(q.at[h], qT.at[h], i, sel)

    def forward(j):
        rel, y, a, b, both = place(j)
        arrived(q.at[:, pl.ds(0, 2 * seg)], rq.at[rel])
        turn_queries(both)

        def low():
            @pl.when(j == 0)
            def _():
                others(0)

        def high(t):
            @pl.when(jnp.logical_and(j == 0, t == (y + 1) // 2 * 2))
            def _():
                others(1)

        phase(y, j, fwd_a, fwd_b, True, low, high)
        for sel, i in both:
            for h in range(heads):
                e = 2 * h + sel
                l = ls[e]
                ob[h, at(i), :] = (acc[e] * (1.0 / l)).astype(bf16).T
                lse[j, e] = ms[e] + jnp.log2(l)
        for sel, i in both:
            for h in range(heads):
                for p in (0, 1):
                    hand(ob.at[h], oo.at[me, h], 2 * i + p, ro)

    def backward(j, last):
        rel, y, a, b, both = place(j)
        arrived(do.at[:, pl.ds(0, 2 * seg)], rdo.at[rel])
        turn_queries(both)
        for h in range(heads):
            for sel, i in both:
                e = 2 * h + sel
                turn(do.at[h], doT.at[h], i, sel)
                lsc[e] = jnp.broadcast_to(lse[j, e], (128, seg)).T
                for r in range(nr):
                    d = jnp.sum(do[h, at(i, r), :].astype(f32) * ob[h, at(i, r), :].astype(f32), axis=1, keepdims=True)
                    dsc[e, r * R:(r + 1) * R, :] = jnp.broadcast_to(d, (R, 128))

        def ready():
            @pl.when(last)
            def _():
                def one(i, _):
                    give_keys(i)
                    return 0

                lax.fori_loop(b, segs, one, 0)

        def done(t):
            for i in (t, t + 1) if t is not segs - 2 else (t,):
                @pl.when(jnp.logical_and(last, i >= y))
                def _():
                    give_keys(i - y)

                @pl.when(i == y)
                def _():
                    give_queries(0, a)

        phase(y, j, bwd_a, bwd_b, False, ready, done)
        give_queries(1, b)

    def turns(s, _):
        is_f = jnp.logical_or(s < 3, s == 4)
        j = jnp.where(s < 3, s, jnp.where(s == 3, 1, jnp.where(s < 6, 3, jnp.where(s == 6, 2, 0))))

        @pl.when(is_f)
        def _():
            forward(j)

        @pl.when(jnp.logical_not(is_f))
        def _():
            backward(j, s == 7)

        return 0

    dkT[...] = jnp.zeros_like(dkT)
    dvT[...] = jnp.zeros_like(dvT)
    keys(0, 0)
    keys(0, 1)
    lax.fori_loop(0, 2 * chips, turns, 0)
    for off in range(1, n):
        sent(insem.at[lax.rem(me + off, n)])
        sent(outsem.at[lax.rem(me + off, n)])
    arrived(oo, ro)
    arrived(dqo, rdq)
    arrived(dko, rdk)
    arrived(dvo, rdv)


def store(*refs):
    sem = refs[-1]
    copies = []
    for i in range(4):
        for b in range(refs[i].shape[0]):
            copies.append(pltpu.make_async_copy(refs[i].at[b], refs[4 + i].at[b], sem.at[i, b]))
    for copy in copies:
        copy.start()
    for copy in copies:
        copy.wait()


def solution(mesh):
    n = mesh.shape["ctx"]
    spec = P("data", "ctx", None, None)

    def local(queries, keys_in, values_in, grad_out):
        batch, shard, heads, dim = queries.shape
        assert batch == n and keys_in.shape[2] == 1
        seq = n * shard
        q, g = (t.transpose(0, 2, 1, 3) for t in (queries, grad_out))
        k, v = (t.reshape(batch, shard, dim) for t in (keys_in, values_in))
        hbm = pl.BlockSpec(memory_space=pl.ANY)
        vm, dma = pltpu.VMEM, pltpu.SemaphoreType.DMA
        wide, thin = vm(q.shape, bf16), vm(k.shape, bf16)
        results = pl.pallas_call(
            functools.partial(kernel, n),
            out_shape=[wide, wide, thin, thin],
            in_specs=[hbm] * 4,
            out_specs=[pl.BlockSpec(memory_space=pltpu.VMEM)] * 4,
            scratch_shapes=[vm((heads, seq, dim), bf16)] * 3 + [vm((seq, dim), bf16)] * 2 + [vm((dim, seq), bf16)] * 2
            + [vm((heads, dim, 2 * shard), bf16)] * 2
            + [vm((2 * heads, dim, shard), f32), vm((2 * heads, 1, shard), f32), vm((2 * heads, 1, shard), f32), vm((n // 2, 2 * heads, 1, shard), f32)]
            + [vm((2 * heads, shard, 128), f32)] * 2 + [vm((dim, seq), f32)] * 2
            + [vm((shard, shard), f32)] * 2 + [vm((1, shard), f32)] * 2 + [vm((shard, shard), bf16)] * 6
            + [dma((n,)), dma((n,)), dma((n,)), dma((n,)), dma((n // 2,)), dma((n // 2,))] + [dma] * 4,
            compiler_params=pltpu.CompilerParams(collective_id=0, has_side_effects=True, vmem_limit_bytes=54400000),
            name="attention",
        )(q, g, k, v)
        o, dq, dk, dv = pl.pallas_call(
            store,
            out_shape=[jax.ShapeDtypeStruct(t.shape, bf16) for t in results],
            in_specs=[hbm] * 4,
            out_specs=[pl.BlockSpec(memory_space=pltpu.HBM)] * 4,
            scratch_shapes=[dma((4, batch))],
            compiler_params=pltpu.CompilerParams(vmem_limit_bytes=1 << 20),
            name="store",
        )(*results)
        o, dq = (t.transpose(0, 2, 1, 3) for t in (o, dq))
        dk, dv = (t.reshape(keys_in.shape) for t in (dk, dv))
        return o, dq, dk, dv

    return jax.shard_map(local, mesh=mesh, in_specs=(spec,) * 4, out_specs=(spec,) * 4, check_vma=False)
```
